16 devices in a mesh: dp: 2 (over z), cp: 8 (over y, x, core).
Axes of the slice: x: 2, y: 2, z: 2, core: 2. Of those that a mesh axis runs over, the one named last changes fastest.
Arguments:
- latent: bfloat16 [32, 6, 96, 512], P(('dp', 'cp')), parts along dimension 0
- conv_kernels: bfloat16 [4, 3, 3, 3, 512, 512], replicated
- conv_biases: float32 [4, 512], replicated
- gn_gammas: float32 [4, 512], replicated
- gn_betas: float32 [4, 512], replicated
Outputs:
- output: bfloat16 [32, 6, 96, 512], P(('dp', 'cp')), parts along dimension 0
There are 2 independent parts. The reference program is written for one: setup_inputs(seed, part) draws one part's arguments, and reference() takes and returns one part's arrays. A program takes and returns all parts, laid end to end along the dimension named above; an argument that names none is the same for every part.
All inputs are finite; a program needn't handle non-finite values.
Results may differ from the reference program's by a relative error of at most 0.0125181.
Values are sent between devices in bfloat16 or wider.
A program may use at most 1 GiB of HBM per device.

```python
import jax
import jax.numpy as jnp
from jax import lax

FRAMES = 16
LAT_HEIGHT = 6
LAT_WIDTH = 96
CHANNELS = 512
GROUPS = 32
NORM_EPS = 1e-6


def setup_inputs(seed: int = 0, part: int = 0) -> dict:
    part_key = jax.random.fold_in(jax.random.key(seed), part)
    key_noise, key_slope, key_jitter, key_gain = jax.random.split(part_key, 4)
    key_kernel, key_bias, key_gamma, key_beta = jax.random.split(jax.random.key(seed + 1), 4)
    time_trend = jnp.linspace(-1.0, 1.0, FRAMES)
    chan_slope = jax.random.normal(key_slope, (CHANNELS,))
    frame_mean = time_trend[:, None] * chan_slope[None, :] + 0.3 * jax.random.normal(key_jitter, (FRAMES, CHANNELS))
    frame_gain = jnp.exp(0.5 * time_trend + 0.2 * jax.random.normal(key_gain, (FRAMES,)))
    base_noise = jax.random.normal(key_noise, (FRAMES, LAT_HEIGHT, LAT_WIDTH, CHANNELS))
    latent = base_noise * frame_gain[:, None, None, None] + frame_mean[:, None, None, :]
    conv_kernels = jax.random.normal(key_kernel, (4, 3, 3, 3, CHANNELS, CHANNELS)) * (27 * CHANNELS) ** -0.5
    conv_biases = 0.3 * jax.random.normal(key_bias, (4, CHANNELS))
    gn_gammas = 1.0 + 0.3 * jax.random.normal(key_gamma, (4, CHANNELS))
    gn_betas = 0.3 * jax.random.normal(key_beta, (4, CHANNELS))
    return {"latent": latent.astype(jnp.bfloat16), "conv_kernels": conv_kernels.astype(jnp.bfloat16), "conv_biases": conv_biases.astype(jnp.float32), "gn_gammas": gn_gammas.astype(jnp.float32), "gn_betas": gn_betas.astype(jnp.float32)}


def norm_act(hidden, gn_gamma, gn_beta):
    widened = hidden.astype(jnp.float32)
    grouped = widened.reshape(hidden.shape[:-1] + (GROUPS, CHANNELS // GROUPS))
    elem_count = grouped.size // GROUPS
    sum_one = jnp.sum(grouped, axis=(0, 1, 2, 4))
    sum_sq = jnp.sum(grouped * grouped, axis=(0, 1, 2, 4))
    grp_mean = sum_one / elem_count
    grp_var = sum_sq / elem_count - grp_mean * grp_mean
    normed = (grouped - grp_mean[:, None]) * lax.rsqrt(grp_var + NORM_EPS)[:, None]
    normed = (normed.reshape(hidden.shape) * gn_gamma + gn_beta).astype(jnp.bfloat16)
    return jax.nn.silu(normed.astype(jnp.float32)).astype(jnp.bfloat16)


def causal_conv(act_in, kernel, conv_bias):
    padded = jnp.concatenate([act_in[:1], act_in[:1], act_in], axis=0).astype(jnp.float32)
    result = lax.conv_general_dilated(padded[None], kernel.astype(jnp.float32), (1, 1, 1), ((0, 0), (1, 1), (1, 1)), dimension_numbers=("NDHWC", "DHWIO", "NDHWC"))[0]
    return (result + conv_bias).astype(jnp.bfloat16)


def reference(latent, conv_kernels, conv_biases, gn_gammas, gn_betas):
    def block_step(hidden, block_params):
        kernel_pair, bias_pair, gamma_pair, beta_pair = block_params
        inner = causal_conv(norm_act(hidden, gamma_pair[0], beta_pair[0]), kernel_pair[0], bias_pair[0])
        inner = causal_conv(norm_act(inner, gamma_pair[1], beta_pair[1]), kernel_pair[1], bias_pair[1])
        return (hidden.astype(jnp.float32) + inner.astype(jnp.float32)).astype(jnp.bfloat16), None

    block_params = (conv_kernels.reshape((2, 2) + conv_kernels.shape[1:]), conv_biases.reshape(2, 2, CHANNELS), gn_gammas.reshape(2, 2, CHANNELS), gn_betas.reshape(2, 2, CHANNELS))
    decoded, _ = lax.scan(block_step, latent, block_params)
    return decoded
```

```python
import jax
import jax.numpy as jnp
from jax import lax
from jax.experimental import pallas as pl
from jax.experimental.pallas import tpu as pltpu
from jax.sharding import PartitionSpec as P

MESH = pl.DeviceIdType.MESH
F32, BF16 = jnp.float32, jnp.bfloat16
GROUPS = 32
NORM_EPS = 1e-6
N_LAYERS = 4
ROWS = 6
WIDTH = 96
LANES = 16
RES = 6
CHANS = 512
TILE = 256


def kernel(n_time, lat_ref, w_ref, bias_ref, gam_ref, bet_ref, out_ref,
           raw, xbuf, acc0, acc1, a0, a1, a2, a3, wbuf, affine, pstat, srecv,
           lat_sem, w_sem, stat_send, stat_recv, halo_send, halo_recv, out_sem):
    me = lax.axis_index("cp")
    nxt = lax.rem(me + 1, n_time)
    acts = (a0, a1, a2, a3)

    barrier = pltpu.get_barrier_semaphore()
    for d in range(1, n_time):
        pl.semaphore_signal(barrier, inc=1, device_id={"cp": lax.rem(me + d, n_time)}, device_id_type=MESH)

    def weights_copy(layer, k):
        slot = lax.rem(layer, 2)
        return pltpu.make_async_copy(w_ref.at[layer, k], wbuf.at[slot, k], w_sem.at[slot, k])

    def halo_copy(frame, par):
        return pltpu.make_async_remote_copy(
            src_ref=raw.at[frame], dst_ref=raw.at[2 + 2 * par + frame],
            send_sem=halo_send.at[frame], recv_sem=halo_recv.at[par, frame],
            device_id={"cp": nxt}, device_id_type=MESH)

    lat_copy = pltpu.make_async_copy(lat_ref, raw.at[pl.ds(0, 2)], lat_sem.at[0])
    x_copy = pltpu.make_async_copy(lat_ref, xbuf, lat_sem.at[1])
    lat_copy.start()
    for k in (2, 1, 0):
        weights_copy(0, k).start()
    x_copy.start()
    lat_copy.wait()
    pl.semaphore_wait(barrier, n_time - 1)

    def cols(c):
        return slice(c * 128, (c + 1) * 128)

    def partial_sums(v):
        folded = v.reshape(v.shape[0] // 8, 8, 128)
        return jnp.sum(folded, axis=0), jnp.sum(folded * folded, axis=0)

    def latent_stats(n, carry):
        frame, row = n // ROWS, lax.rem(n, ROWS)
        new = []
        for c in range(4):
            s1, s2 = partial_sums(raw[frame, row, :, cols(c)].astype(F32))
            new += [carry[2 * c] + s1, carry[2 * c + 1] + s2]
        return tuple(new)

    sums = lax.fori_loop(0, 2 * ROWS, latent_stats, tuple(jnp.zeros((8, 128), F32) for _ in range(8)))
    for c in range(4):
        pstat[c] = sums[2 * c]
        pstat[4 + c] = sums[2 * c + 1]
    x_copy.wait()

    elem_count = float(n_time * 2 * ROWS * WIDTH * (CHANS // GROUPS))
    lane = lax.broadcasted_iota(jnp.int32, (8, 128), 1)
    sub16 = lax.broadcasted_iota(jnp.int32, (LANES, 128), 0)

    def exchange(layer, par):
        for n in range(8):
            srecv[par, me, n:n + 1, :] = jnp.sum(pstat[n], axis=0, keepdims=True)
        def stat_copy(d):
            return pltpu.make_async_remote_copy(
                src_ref=srecv.at[par, me], dst_ref=srecv.at[par, me],
                send_sem=stat_send.at[d], recv_sem=stat_recv.at[par, me],
                device_id={"cp": lax.rem(me + d, n_time)}, device_id_type=MESH)
        for d in range(1, n_time):
            stat_copy(d).start()

        @pl.when(layer == 0)
        def _():
            halo_copy(1, par).start()

        halo_copy(0, par).start()
        for d in range(1, n_time):
            src = lax.rem(me + n_time - d, n_time)
            pltpu.make_async_remote_copy(
                src_ref=srecv.at[par, src], dst_ref=srecv.at[par, src],
                send_sem=stat_send.at[d], recv_sem=stat_recv.at[par, src],
                device_id={"cp": src}, device_id_type=MESH).wait_recv()
        total = srecv[par, 0]
        for n in range(1, n_time):
            total = total + srecv[par, n]
        for s in (1, 2, 4, 8):
            total = total + jnp.where((lane & s) == 0, pltpu.roll(total, 128 - s, 1), pltpu.roll(total, s, 1))
        grp_mean = total[0:4] / elem_count
        grp_var = total[4:8] / elem_count - grp_mean * grp_mean
        scale = lax.rsqrt(grp_var + NORM_EPS) * gam_ref[layer]
        affine[0:4, :] = scale
        affine[4:8, :] = bet_ref[layer] - grp_mean * scale
        for d in range(1, n_time):
            stat_copy(d).wait_send()

    def norm_row(slot, row, dst):
        for c in range(4):
            v = raw[slot, row, :, cols(c)].astype(F32)
            u = (v * affine[c:c + 1, :] + affine[4 + c:5 + c, :]).astype(BF16).astype(F32)
            act = u * jax.nn.sigmoid(u)
            dst[row, LANES:LANES + WIDTH, cols(c)] = act.astype(BF16)
            before = pltpu.roll(act[WIDTH - LANES:], 1, 0)
            dst[row, 0:LANES, cols(c)] = jnp.where(sub16 == 0, 0.0, before).astype(BF16)
            after = pltpu.roll(act[:LANES], LANES - 1, 0)
            dst[row, LANES + WIDTH:, cols(c)] = jnp.where(sub16 == LANES - 1, 0.0, after).astype(BF16)

    def group(acc, act, w_slot, k, first, side=()):
        for s, di in enumerate((1, 0, 2)):
            lo, hi = max(0, 1 - di), min(ROWS, ROWS + 1 - di)
            lhs = jnp.concatenate(
                [act[lo + di - 1:hi + di - 1, LANES * dj:LANES * dj + WIDTH, :].reshape((hi - lo) * WIDTH, CHANS)
                 for dj in range(3)], axis=1)
            part = jnp.dot(lhs, wbuf[w_slot, k, di].reshape(3 * CHANS, CHANS), preferred_element_type=F32)
            part = part.reshape(hi - lo, WIDTH, CHANS)
            if first and s == 0:
                acc[...] = part
            else:
                acc[lo:hi] = acc[lo:hi] + part
            for step in side[s] if side else ():
                step()

    def epilogue(frame, row, acc, layer, odd, sums):
        for q in range(2):
            for half in range(2):
                c = 2 * q + half
                h = (acc[row, :, cols(c)] + bias_ref[layer, :, cols(c)]).astype(BF16).astype(F32)
                x_old = xbuf[frame, row, :, cols(c)].astype(F32)
                res = (jnp.where(odd, x_old, 0.0) + h).astype(BF16)
                wide = res.astype(F32)
                raw[frame, row, :, cols(c)] = res
                xbuf[frame, row, :, cols(c)] = jnp.where(odd, wide, x_old).astype(BF16)
                s1, s2 = partial_sums(wide)
                sums[c] = s1 if sums[c] is None else sums[c] + s1
                sums[4 + c] = s2 if sums[4 + c] is None else sums[4 + c] + s2

    def layer_body(layer, carry):
        par = lax.rem(layer, 2)
        odd = par == 1
        more = layer + 1 < N_LAYERS
        halo_0 = jnp.where(me == 0, 0, 2 + 2 * par)
        halo_1 = jnp.where(me == 0, 0, 3 + 2 * par)

        exchange(layer, par)
        for k in (2, 1, 0):
            weights_copy(layer, k).wait()

        @pl.when(more)
        def _():
            for k in (2, 1, 0):
                weights_copy(layer + 1, k).start()

        for row in range(ROWS):
            norm_row(1, row, a3)

        def spread(fn):
            return [[lambda r=r: fn(r) for r in (2 * n, 2 * n + 1)] for n in range(3)]

        group(acc1, a3, par, 2, True, spread(lambda r: norm_row(0, r, a2)))
        halo_copy(1, par).wait_recv()
        group(acc1, a2, par, 1, False, spread(lambda r: norm_row(halo_1, r, a1)))
        halo_copy(1, par).wait_send()
        group(acc1, a1, par, 0, False)

        def finish_frame_1():
            sums = [None] * 8
            for row in range(ROWS):
                epilogue(1, row, acc1, layer, odd, sums)
            for n in range(8):
                pstat[n] = sums[n]

            @pl.when(more)
            def _():
                halo_copy(1, 1 - par).start()

        group(acc0, a2, par, 2, True, [[finish_frame_1], [], []])
        halo_copy(0, par).wait()
        group(acc0, a1, par, 1, False, spread(lambda r: norm_row(halo_0, r, a0)))
        group(acc0, a0, par, 0, False)
        sums = [None] * 8
        for row in range(ROWS):
            epilogue(0, row, acc0, layer, odd, sums)
        for n in range(8):
            pstat[n] = pstat[n] + sums[n]
        return carry

    lax.fori_loop(0, N_LAYERS, layer_body, 0)

    out_copy = pltpu.make_async_copy(raw.at[pl.ds(0, 2)], out_ref, out_sem)
    out_copy.start()
    out_copy.wait()


def solution(mesh):
    n_time = mesh.shape["cp"]
    frame_spec = P(("dp", "cp"))

    def local_fn(latent, conv_kernels, conv_biases, gn_gammas, gn_betas):
        lat = latent.reshape(2, ROWS, LANES, RES, CHANS).transpose(0, 1, 3, 2, 4).reshape(2, ROWS, WIDTH, CHANS)
        act = pltpu.VMEM((ROWS, WIDTH + 2 * LANES, CHANS), BF16)
        any_spec = pl.BlockSpec(memory_space=pl.ANY)
        vmem_spec = pl.BlockSpec(memory_space=pltpu.VMEM)

        def run(*refs):
            return kernel(n_time, *refs)

        out = pl.pallas_call(
            run,
            out_shape=jax.ShapeDtypeStruct((2, ROWS, WIDTH, CHANS), BF16),
            in_specs=[any_spec, any_spec, vmem_spec, vmem_spec, vmem_spec],
            out_specs=any_spec,
            scratch_shapes=[
                pltpu.VMEM((6, ROWS, WIDTH, CHANS), BF16),
                pltpu.VMEM((2, ROWS, WIDTH, CHANS), BF16),
                pltpu.VMEM((ROWS, WIDTH, CHANS), F32),
                pltpu.VMEM((ROWS, WIDTH, CHANS), F32),
                act, act, act, act,
                pltpu.VMEM((2, 3, 3, 3, CHANS, CHANS), BF16),
                pltpu.VMEM((8, 128), F32),
                pltpu.VMEM((8, 8, 128), F32),
                pltpu.VMEM((2, n_time, 8, 128), F32),
                pltpu.SemaphoreType.DMA((2,)),
                pltpu.SemaphoreType.DMA((2, 3)),
                pltpu.SemaphoreType.DMA((n_time,)),
                pltpu.SemaphoreType.DMA((2, n_time)),
                pltpu.SemaphoreType.DMA((2,)),
                pltpu.SemaphoreType.DMA((2, 2)),
                pltpu.SemaphoreType.DMA,
            ],
            compiler_params=pltpu.CompilerParams(
                collective_id=0, has_side_effects=True, vmem_limit_bytes=60 * 1024 * 1024),
            name="resnet_blocks",
        )(lat, conv_kernels, conv_biases.reshape(N_LAYERS, 1, CHANS),
          gn_gammas.reshape(N_LAYERS, 4, 128), gn_betas.reshape(N_LAYERS, 4, 128))
        return out.reshape(2, ROWS, RES, LANES, CHANS).transpose(0, 1, 3, 2, 4).reshape(2, ROWS, WIDTH, CHANS)

    return jax.shard_map(local_fn, mesh=mesh, in_specs=(frame_spec, P(), P(), P(), P()), out_specs=frame_spec, check_vma=False)
```

```python
import jax
import jax.numpy as jnp
from jax import lax
from jax.experimental import pallas as pl
from jax.experimental.pallas import tpu as pltpu
from jax.sharding import PartitionSpec as P

MESH = pl.DeviceIdType.MESH
F32, BF16 = jnp.float32, jnp.bfloat16
GROUPS = 32
NORM_EPS = 1e-6
N_LAYERS = 4
ROWS = 6
WIDTH = 96
LANES = 16
RES = 6
CHANS = 512
TILE = 256


def kernel(n_time, lat_ref, w_ref, bias_ref, gam_ref, bet_ref, out_ref,
           raw, xbuf, acc0, acc1, a0, a1, a2, a3, wbuf, perm, params, affine, pstat, srecv,
           lat_sem, w_sem, stat_send, stat_recv, halo_send, halo_recv):
    me = lax.axis_index("cp")
    nxt = lax.rem(me + 1, n_time)
    acts = (a0, a1, a2, a3)

    barrier = pltpu.get_barrier_semaphore()
    for d in range(1, n_time):
        pl.semaphore_signal(barrier, inc=1, device_id={"cp": lax.rem(me + d, n_time)}, device_id_type=MESH)

    def weights_copy(layer, k):
        slot = lax.rem(layer, 2)
        return pltpu.make_async_copy(w_ref.at[layer, k], wbuf.at[slot, k], w_sem.at[slot, k])

    def halo_copy(frame, par):
        return pltpu.make_async_remote_copy(
            src_ref=raw.at[frame], dst_ref=raw.at[2 + 2 * par + frame],
            send_sem=halo_send.at[frame], recv_sem=halo_recv.at[par, frame],
            device_id={"cp": nxt}, device_id_type=MESH)

    lat_copy = pltpu.make_async_copy(lat_ref, out_ref, lat_sem)
    lat_copy.start()
    weights_copy(0, 2).start()
    for n, ref in enumerate((bias_ref, gam_ref, bet_ref)):
        for layer in range(N_LAYERS):
            params[n, layer] = ref[layer:layer + 1, :]

    def cols(c):
        return slice(c * 128, (c + 1) * 128)

    def partial_sums(v):
        folded = v.reshape(v.shape[0] // 8, 8, 128)
        return jnp.sum(folded, axis=0), jnp.sum(folded * folded, axis=0)

    def load_latent(n, carry):
        frame, row = n // ROWS, lax.rem(n, ROWS)
        new = list(carry)
        for c in range(4):
            perm[c] = out_ref[frame, row, :, cols(c)].astype(F32)
            for r in range(RES):
                v = perm[c, pl.ds(r, LANES, stride=RES), :]
                here = (frame, row, slice(r * LANES, (r + 1) * LANES), cols(c))
                raw[here] = v.astype(BF16)
                xbuf[here] = v.astype(BF16)
                s1, s2 = partial_sums(v)
                new[2 * c] = new[2 * c] + s1
                new[2 * c + 1] = new[2 * c + 1] + s2
        return tuple(new)

    lat_copy.wait()
    sums = lax.fori_loop(0, 2 * ROWS, load_latent, tuple(jnp.zeros((8, 128), F32) for _ in range(8)))
    for c in range(4):
        pstat[c] = sums[2 * c]
        pstat[4 + c] = sums[2 * c + 1]
    pl.semaphore_wait(barrier, n_time - 1)

    elem_count = float(n_time * 2 * ROWS * WIDTH * (CHANS // GROUPS))
    lane = lax.broadcasted_iota(jnp.int32, (8, 128), 1)
    sub16 = lax.broadcasted_iota(jnp.int32, (LANES, 128), 0)

    def exchange(layer, par):
        for n in range(8):
            srecv[par, me, n:n + 1, :] = jnp.sum(pstat[n], axis=0, keepdims=True)
        def stat_copy(d):
            return pltpu.make_async_remote_copy(
                src_ref=srecv.at[par, me], dst_ref=srecv.at[par, me],
                send_sem=stat_send.at[d], recv_sem=stat_recv.at[par, me],
                device_id={"cp": lax.rem(me + d, n_time)}, device_id_type=MESH)
        for d in range(1, n_time):
            stat_copy(d).start()

        @pl.when(layer == 0)
        def _():
            weights_copy(0, 1).start()
            weights_copy(0, 0).start()

        for d in range(1, n_time):
            src = lax.rem(me + n_time - d, n_time)
            pltpu.make_async_remote_copy(
                src_ref=srecv.at[par, src], dst_ref=srecv.at[par, src],
                send_sem=stat_send.at[d], recv_sem=stat_recv.at[par, src],
                device_id={"cp": src}, device_id_type=MESH).wait_recv()

        @pl.when(layer == 0)
        def _():
            halo_copy(1, par).start()

        halo_copy(0, par).start()
        total = srecv[par, 0]
        for n in range(1, n_time):
            total = total + srecv[par, n]
        for s in (1, 2, 4, 8):
            total = total + jnp.where((lane & s) == 0, pltpu.roll(total, 128 - s, 1), pltpu.roll(total, s, 1))
        grp_mean = total[0:4] / elem_count
        grp_var = total[4:8] / elem_count - grp_mean * grp_mean
        inv = lax.rsqrt(grp_var + NORM_EPS)
        for c in range(4):
            scale = inv[c:c + 1] * params[1, layer, :, cols(c)]
            affine[c:c + 1, :] = scale
            affine[4 + c:5 + c, :] = params[2, layer, :, cols(c)] - grp_mean[c:c + 1] * scale
        for d in range(1, n_time):
            stat_copy(d).wait_send()

    def norm_row(slot, row, dst):
        for c in range(4):
            v = raw[slot, row, :, cols(c)].astype(F32)
            u = (v * affine[c:c + 1, :] + affine[4 + c:5 + c, :]).astype(BF16).astype(F32)
            act = u * jax.nn.sigmoid(u)
            dst[row, LANES:LANES + WIDTH, cols(c)] = act.astype(BF16)
            before = pltpu.roll(act[WIDTH - LANES:], 1, 0)
            dst[row, 0:LANES, cols(c)] = jnp.where(sub16 == 0, 0.0, before).astype(BF16)
            after = pltpu.roll(act[:LANES], LANES - 1, 0)
            dst[row, LANES + WIDTH:, cols(c)] = jnp.where(sub16 == LANES - 1, 0.0, after).astype(BF16)

    def group(acc, act, w_slot, k, first, side=()):
        for s, di in enumerate((1, 0, 2)):
            lo, hi = max(0, 1 - di), min(ROWS, ROWS + 1 - di)
            lhs = jnp.concatenate(
                [act[lo + di - 1:hi + di - 1, LANES * dj:LANES * dj + WIDTH, :].reshape((hi - lo) * WIDTH, CHANS)
                 for dj in range(3)], axis=1)
            part = jnp.dot(lhs, wbuf[w_slot, k, di].reshape(3 * CHANS, CHANS), preferred_element_type=F32)
            part = part.reshape(hi - lo, WIDTH, CHANS)
            if first and s == 0:
                acc[...] = part
            else:
                acc[lo:hi] = acc[lo:hi] + part
            for step in side[s] if side else ():
                step()

    def epilogue(frame, row, acc, layer, odd, sums):
        for q in range(2):
            for half in range(2):
                c = 2 * q + half
                h = (acc[row, :, cols(c)] + params[0, layer, :, cols(c)]).astype(BF16).astype(F32)
                x_old = xbuf[frame, row, :, cols(c)].astype(F32)
                res = (jnp.where(odd, x_old, 0.0) + h).astype(BF16)
                wide = res.astype(F32)
                raw[frame, row, :, cols(c)] = res
                xbuf[frame, row, :, cols(c)] = jnp.where(odd, wide, x_old).astype(BF16)
                s1, s2 = partial_sums(wide)
                sums[c] = s1 if sums[c] is None else sums[c] + s1
                sums[4 + c] = s2 if sums[4 + c] is None else sums[4 + c] + s2

    def layer_body(layer, carry):
        par = lax.rem(layer, 2)
        odd = par == 1
        more = layer + 1 < N_LAYERS
        halo_0 = jnp.where(me == 0, 0, 2 + 2 * par)
        halo_1 = jnp.where(me == 0, 0, 3 + 2 * par)

        exchange(layer, par)
        for k in (2, 1, 0):
            weights_copy(layer, k).wait()

        @pl.when(more)
        def _():
            for k in (2, 1, 0):
                weights_copy(layer + 1, k).start()

        for row in range(ROWS):
            norm_row(1, row, a3)

        def spread(fn):
            return [[lambda r=r: fn(r) for r in (2 * n, 2 * n + 1)] for n in range(3)]

        group(acc1, a3, par, 2, True, spread(lambda r: norm_row(0, r, a2)))
        halo_copy(1, par).wait_recv()
        group(acc1, a2, par, 1, False, spread(lambda r: norm_row(halo_1, r, a1)))
        halo_copy(1, par).wait_send()
        group(acc1, a1, par, 0, False)

        def finish_frame_1():
            sums = [None] * 8
            for row in range(ROWS):
                epilogue(1, row, acc1, layer, odd, sums)
            for n in range(8):
                pstat[n] = sums[n]

            @pl.when(more)
            def _():
                halo_copy(1, 1 - par).start()

        group(acc0, a2, par, 2, True, [[finish_frame_1], [], []])
        halo_copy(0, par).wait()
        group(acc0, a1, par, 1, False, spread(lambda r: norm_row(halo_0, r, a0)))
        group(acc0, a0, par, 0, False)
        sums = [None] * 8
        for row in range(ROWS):
            epilogue(0, row, acc0, layer, odd, sums)
        for n in range(8):
            pstat[n] = pstat[n] + sums[n]
        return carry

    lax.fori_loop(0, N_LAYERS, layer_body, 0)

    def store_row(n, carry):
        frame, row = n // ROWS, lax.rem(n, ROWS)
        for c in range(4):
            for r in range(RES):
                perm[c, pl.ds(r, LANES, stride=RES), :] = raw[frame, row, r * LANES:(r + 1) * LANES, cols(c)].astype(F32)
            out_ref[frame, row, :, cols(c)] = perm[c].astype(BF16)
        return carry

    lax.fori_loop(0, 2 * ROWS, store_row, 0)


def solution(mesh):
    n_time = mesh.shape["cp"]
    frame_spec = P(("dp", "cp"))

    def local_fn(latent, conv_kernels, conv_biases, gn_gammas, gn_betas):
        act = pltpu.VMEM((ROWS, WIDTH + 2 * LANES, CHANS), BF16)
        any_spec = pl.BlockSpec(memory_space=pl.ANY)
        vmem_spec = pl.BlockSpec(memory_space=pltpu.VMEM)

        def run(*refs):
            return kernel(n_time, *refs)

        return pl.pallas_call(
            run,
            out_shape=jax.ShapeDtypeStruct((2, ROWS, WIDTH, CHANS), BF16),
            in_specs=[any_spec, any_spec, vmem_spec, vmem_spec, vmem_spec],
            out_specs=vmem_spec,
            scratch_shapes=[
                pltpu.VMEM((6, ROWS, WIDTH, CHANS), BF16),
                pltpu.VMEM((2, ROWS, WIDTH, CHANS), BF16),
                pltpu.VMEM((ROWS, WIDTH, CHANS), F32),
                pltpu.VMEM((ROWS, WIDTH, CHANS), F32),
                act, act, act, act,
                pltpu.VMEM((2, 3, 3, 3, CHANS, CHANS), BF16),
                pltpu.VMEM((4, WIDTH, 128), F32),
                pltpu.VMEM((3, N_LAYERS, 1, CHANS), F32),
                pltpu.VMEM((8, 128), F32),
                pltpu.VMEM((8, 8, 128), F32),
                pltpu.VMEM((2, n_time, 8, 128), F32),
                pltpu.SemaphoreType.DMA,
                pltpu.SemaphoreType.DMA((2, 3)),
                pltpu.SemaphoreType.DMA((n_time,)),
                pltpu.SemaphoreType.DMA((2, n_time)),
                pltpu.SemaphoreType.DMA((2,)),
                pltpu.SemaphoreType.DMA((2, 2)),
            ],
            compiler_params=pltpu.CompilerParams(
                collective_id=0, has_side_effects=True, vmem_limit_bytes=60 * 1024 * 1024),
            name="resnet_blocks",
        )(latent, conv_kernels, conv_biases, gn_gammas, gn_betas)

    return jax.shard_map(local_fn, mesh=mesh, in_specs=(frame_spec, P(), P(), P(), P()), out_specs=frame_spec, check_vma=False)
```

```python
import jax
import jax.numpy as jnp
from jax import lax
from jax.experimental import pallas as pl
from jax.experimental.pallas import tpu as pltpu
from jax.sharding import PartitionSpec as P

MESH = pl.DeviceIdType.MESH
F32, BF16 = jnp.float32, jnp.bfloat16
GROUPS = 32
NORM_EPS = 1e-6
N_LAYERS = 4
ROWS = 6
WIDTH = 96
LANES = 16
RES = 6
CHANS = 512
TILE = 256


def kernel(n_time, lat_ref, w_ref, bias_ref, gam_ref, bet_ref, out_ref,
           raw, xbuf, acc0, acc1, a0, a1, a2, a3, wbuf, perm, params, affine, pstat, srecv,
           lat_sem, w_sem, stat_send, stat_recv, halo_send, halo_recv):
    me = lax.axis_index("cp")
    nxt = lax.rem(me + 1, n_time)
    acts = (a0, a1, a2, a3)

    barrier = pltpu.get_barrier_semaphore()
    for d in range(1, n_time):
        pl.semaphore_signal(barrier, inc=1, device_id={"cp": lax.rem(me + d, n_time)}, device_id_type=MESH)

    def weights_copy(layer, k):
        slot = lax.rem(layer, 2)
        return pltpu.make_async_copy(w_ref.at[layer, k], wbuf.at[slot, k], w_sem.at[slot, k])

    def halo_copy(frame, par):
        return pltpu.make_async_remote_copy(
            src_ref=raw.at[frame], dst_ref=raw.at[2 + 2 * par + frame],
            send_sem=halo_send.at[frame], recv_sem=halo_recv.at[par, frame],
            device_id={"cp": nxt}, device_id_type=MESH)

    lat_copy = pltpu.make_async_copy(lat_ref, out_ref, lat_sem)
    lat_copy.start()
    weights_copy(0, 2).start()
    for n, ref in enumerate((bias_ref, gam_ref, bet_ref)):
        for layer in range(N_LAYERS):
            params[n, layer] = ref[layer:layer + 1, :]

    def cols(c):
        return slice(c * 128, (c + 1) * 128)

    def partial_sums(v):
        folded = v.reshape(v.shape[0] // 8, 8, 128)
        return jnp.sum(folded, axis=0), jnp.sum(folded * folded, axis=0)

    def latent_sums(n, carry):
        frame, row = n // ROWS, lax.rem(n, ROWS)
        new = []
        for c in range(4):
            s1, s2 = partial_sums(out_ref[frame, row, :, cols(c)].astype(F32))
            new += [carry[2 * c] + s1, carry[2 * c + 1] + s2]
        return tuple(new)

    def permute_latent(n, carry):
        frame, row = n // ROWS, lax.rem(n, ROWS)
        for c in range(4):
            perm[c] = out_ref[frame, row, :, cols(c)].astype(F32)
            for r in range(RES):
                v = perm[c, pl.ds(r, LANES, stride=RES), :].astype(BF16)
                here = (frame, row, slice(r * LANES, (r + 1) * LANES), cols(c))
                raw[here] = v
                xbuf[here] = v
        return carry

    lat_copy.wait()
    sums = lax.fori_loop(0, 2 * ROWS, latent_sums, tuple(jnp.zeros((8, 128), F32) for _ in range(8)))
    for c in range(4):
        pstat[c] = sums[2 * c]
        pstat[4 + c] = sums[2 * c + 1]

    elem_count = float(n_time * 2 * ROWS * WIDTH * (CHANS // GROUPS))
    lane = lax.broadcasted_iota(jnp.int32, (8, 128), 1)
    sub16 = lax.broadcasted_iota(jnp.int32, (LANES, 128), 0)

    def stat_copy(par, d):
        return pltpu.make_async_remote_copy(
            src_ref=srecv.at[par, me], dst_ref=srecv.at[par, me],
            send_sem=stat_send.at[d], recv_sem=stat_recv.at[par, me],
            device_id={"cp": lax.rem(me + d, n_time)}, device_id_type=MESH)

    def sums_out(par):
        for n in range(8):
            srecv[par, me, n:n + 1, :] = jnp.sum(pstat[n], axis=0, keepdims=True)
        for d in range(1, n_time):
            stat_copy(par, d).start()

    def sums_in(layer, par):

        for d in range(1, n_time):
            src = lax.rem(me + n_time - d, n_time)
            pltpu.make_async_remote_copy(
                src_ref=srecv.at[par, src], dst_ref=srecv.at[par, src],
                send_sem=stat_send.at[d], recv_sem=stat_recv.at[par, src],
                device_id={"cp": src}, device_id_type=MESH).wait_recv()

        @pl.when(layer == 0)
        def _():
            halo_copy(1, par).start()

        halo_copy(0, par).start()
        total = srecv[par, 0]
        for n in range(1, n_time):
            total = total + srecv[par, n]
        for s in (1, 2, 4, 8):
            total = total + jnp.where((lane & s) == 0, pltpu.roll(total, 128 - s, 1), pltpu.roll(total, s, 1))
        grp_mean = total[0:4] / elem_count
        grp_var = total[4:8] / elem_count - grp_mean * grp_mean
        inv = lax.rsqrt(grp_var + NORM_EPS)
        for c in range(4):
            scale = inv[c:c + 1] * params[1, layer, :, cols(c)]
            affine[c:c + 1, :] = scale
            affine[4 + c:5 + c, :] = params[2, layer, :, cols(c)] - grp_mean[c:c + 1] * scale
        for d in range(1, n_time):
            stat_copy(par, d).wait_send()

    pl.semaphore_wait(barrier, n_time - 1)
    sums_out(0)
    weights_copy(0, 1).start()
    weights_copy(0, 0).start()
    lax.fori_loop(0, 2 * ROWS, permute_latent, 0)

    def norm_row(slot, row, dst):
        for c in range(4):
            v = raw[slot, row, :, cols(c)].astype(F32)
            u = (v * affine[c:c + 1, :] + affine[4 + c:5 + c, :]).astype(BF16).astype(F32)
            act = u * jax.nn.sigmoid(u)
            dst[row, LANES:LANES + WIDTH, cols(c)] = act.astype(BF16)
            before = pltpu.roll(act[WIDTH - LANES:], 1, 0)
            dst[row, 0:LANES, cols(c)] = jnp.where(sub16 == 0, 0.0, before).astype(BF16)
            after = pltpu.roll(act[:LANES], LANES - 1, 0)
            dst[row, LANES + WIDTH:, cols(c)] = jnp.where(sub16 == LANES - 1, 0.0, after).astype(BF16)

    def group(acc, act, w_slot, k, first, side=None, parts=1):
        side = side or {}
        height = ROWS // parts
        steps = [(part, di) for part in range(parts) for di in (1, 0, 2)]
        for n, (part, di) in enumerate(steps):
            lo, hi = max(height * part, 1 - di), min(height * (part + 1), ROWS + 1 - di)
            lhs = jnp.concatenate(
                [act[lo + di - 1:hi + di - 1, LANES * dj:LANES * dj + WIDTH, :].reshape((hi - lo) * WIDTH, CHANS)
                 for dj in range(3)], axis=1)
            prod = jnp.dot(lhs, wbuf[w_slot, k, di].reshape(3 * CHANS, CHANS), preferred_element_type=F32)
            prod = prod.reshape(hi - lo, WIDTH, CHANS)
            if first and di == 1:
                acc[lo:hi] = prod
            else:
                acc[lo:hi] = acc[lo:hi] + prod
            for step in side.get(n, ()):
                step()

    def epilogue(frame, row, acc, layer, odd, sums):
        for q in range(2):
            for half in range(2):
                c = 2 * q + half
                h = (acc[row, :, cols(c)] + params[0, layer, :, cols(c)]).astype(BF16).astype(F32)
                x_old = xbuf[frame, row, :, cols(c)].astype(F32)
                res = (jnp.where(odd, x_old, 0.0) + h).astype(BF16)
                wide = res.astype(F32)
                raw[frame, row, :, cols(c)] = res
                xbuf[frame, row, :, cols(c)] = jnp.where(odd, wide, x_old).astype(BF16)
                s1, s2 = partial_sums(wide)
                sums[c] = s1 if sums[c] is None else sums[c] + s1
                sums[4 + c] = s2 if sums[4 + c] is None else sums[4 + c] + s2

    def layer_body(layer, carry):
        par = lax.rem(layer, 2)
        odd = par == 1
        more = layer + 1 < N_LAYERS
        later = layer > 0
        halo_0 = jnp.where(me == 0, 0, 2 + 2 * par)
        halo_1 = jnp.where(me == 0, 0, 3 + 2 * par)

        sums_in(layer, par)
        for k in (2, 1, 0):
            weights_copy(layer, k).wait()

        @pl.when(more)
        def _():
            for k in (2, 1, 0):
                weights_copy(layer + 1, k).start()

        for row in range(4):
            norm_row(1, row, a3)

        def normed(slot, dst, plan):
            return {n: [lambda r=r: norm_row(slot, r, dst) for r in rows] for n, rows in plan.items()}

        def finished(frame, acc, sums, plan):
            return {n: [lambda r=r: epilogue(frame, r, acc, layer, odd, sums) for r in rows] for n, rows in plan.items()}

        side = normed(0, a2, {1: (0,), 2: (1,), 3: (2,), 4: (3, 4), 5: (5,)})
        side[0] = [lambda r=r: norm_row(1, r, a3) for r in (4, 5)]
        group(acc1, a3, par, 2, True, side, 2)
        @pl.when(later)
        def _():
            halo_copy(1, par).wait_recv()

        group(acc1, a2, par, 1, False, normed(jnp.where(later, halo_1, 0), a1, {0: (0, 1), 1: (2, 3), 2: (4, 5)}))

        @pl.when(layer == 0)
        def _():
            halo_copy(1, par).wait_recv()

            def row_step(row, carry):
                norm_row(halo_1, row, a1)
                return carry

            lax.fori_loop(0, ROWS, row_step, 0)

        halo_copy(1, par).wait_send()
        sums = [None] * 8
        group(acc1, a1, par, 0, False, finished(1, acc1, sums, {3: (0,), 4: (1,), 5: (2,)}), 2)

        def finish_frame_1():
            for row in (3, 4, 5):
                epilogue(1, row, acc1, layer, odd, sums)
            for n in range(8):
                pstat[n] = sums[n]

            @pl.when(more)
            def _():
                halo_copy(1, 1 - par).start()

        group(acc0, a2, par, 2, True, {0: [finish_frame_1]})
        halo_copy(0, par).wait()
        group(acc0, a1, par, 1, False, normed(halo_0, a0, {0: (0, 1), 1: (2, 3), 2: (4, 5)}))
        sums_0 = [None] * 8
        group(acc0, a0, par, 0, False, finished(0, acc0, sums_0, {3: (0,), 4: (1,), 5: (2,)}), 2)
        for row in (3, 4, 5):
            epilogue(0, row, acc0, layer, odd, sums_0)
        for n in range(8):
            pstat[n] = pstat[n] + sums_0[n]

        @pl.when(more)
        def _():
            sums_out(1 - par)

        return carry

    lax.fori_loop(0, N_LAYERS, layer_body, 0)

    out_ref[...] = raw[0:2]


def unpermute(in_ref, out_ref, perm, rows, sems):
    def cols(c):
        return slice(c * 128, (c + 1) * 128)

    def row_copy(n):
        return pltpu.make_async_copy(rows.at[n], out_ref.at[n // ROWS, n % ROWS], sems.at[n])

    def store_row(n, carry):
        frame, row = n // ROWS, lax.rem(n, ROWS)
        for c in range(4):
            for r in range(RES):
                perm[c, pl.ds(r, LANES, stride=RES), :] = in_ref[frame, row, r * LANES:(r + 1) * LANES, cols(c)].astype(F32)
            rows[n, :, cols(c)] = perm[c].astype(BF16)
        row_copy(n).start()
        return carry

    lax.fori_loop(0, 2 * ROWS, store_row, 0)
    for n in range(2 * ROWS):
        row_copy(n).wait()


def solution(mesh):
    n_time = mesh.shape["cp"]
    frame_spec = P(("dp", "cp"))

    def local_fn(latent, conv_kernels, conv_biases, gn_gammas, gn_betas):
        act = pltpu.VMEM((ROWS, WIDTH + 2 * LANES, CHANS), BF16)
        any_spec = pl.BlockSpec(memory_space=pl.ANY)
        vmem_spec = pl.BlockSpec(memory_space=pltpu.VMEM)

        def run(*refs):
            return kernel(n_time, *refs)

        permuted = pl.pallas_call(
            run,
            out_shape=jax.ShapeDtypeStruct((2, ROWS, WIDTH, CHANS), BF16),
            in_specs=[any_spec, any_spec, vmem_spec, vmem_spec, vmem_spec],
            out_specs=vmem_spec,
            scratch_shapes=[
                pltpu.VMEM((6, ROWS, WIDTH, CHANS), BF16),
                pltpu.VMEM((2, ROWS, WIDTH, CHANS), BF16),
                pltpu.VMEM((ROWS, WIDTH, CHANS), F32),
                pltpu.VMEM((ROWS, WIDTH, CHANS), F32),
                act, act, act, act,
                pltpu.VMEM((2, 3, 3, 3, CHANS, CHANS), BF16),
                pltpu.VMEM((4, WIDTH, 128), F32),
                pltpu.VMEM((3, N_LAYERS, 1, CHANS), F32),
                pltpu.VMEM((8, 128), F32),
                pltpu.VMEM((8, 8, 128), F32),
                pltpu.VMEM((2, n_time, 8, 128), F32),
                pltpu.SemaphoreType.DMA,
                pltpu.SemaphoreType.DMA((2, 3)),
                pltpu.SemaphoreType.DMA((n_time,)),
                pltpu.SemaphoreType.DMA((2, n_time)),
                pltpu.SemaphoreType.DMA((2,)),
                pltpu.SemaphoreType.DMA((2, 2)),
            ],
            compiler_params=pltpu.CompilerParams(
                collective_id=0, has_side_effects=True, vmem_limit_bytes=60 * 1024 * 1024),
            name="resnet_blocks",
        )(latent, conv_kernels, conv_biases, gn_gammas, gn_betas)
        return pl.pallas_call(
            unpermute,
            out_shape=jax.ShapeDtypeStruct((2, ROWS, WIDTH, CHANS), BF16),
            in_specs=[vmem_spec],
            out_specs=any_spec,
            scratch_shapes=[
                pltpu.VMEM((4, WIDTH, 128), F32),
                pltpu.VMEM((2 * ROWS, WIDTH, CHANS), BF16),
                pltpu.SemaphoreType.DMA((2 * ROWS,)),
            ],
            name="unpermute",
        )(permuted)

    return jax.shard_map(local_fn, mesh=mesh, in_specs=(frame_spec, P(), P(), P(), P()), out_specs=frame_spec, check_vma=False)
```

```python
import jax
import jax.numpy as jnp
from jax import lax
from jax.experimental import pallas as pl
from jax.experimental.pallas import tpu as pltpu
from jax.sharding import PartitionSpec as P

MESH = pl.DeviceIdType.MESH
F32, BF16 = jnp.float32, jnp.bfloat16
GROUPS = 32
NORM_EPS = 1e-6
N_LAYERS = 4
ROWS = 6
WIDTH = 96
LANES = 16
RES = 6
CHANS = 512
TILE = 256


def kernel(n_time, lat_ref, w_ref, bias_ref, gam_ref, bet_ref, out_ref,
           raw, xbuf, acc0, acc1, a0, a1, a2, a3, wbuf, perm, params, affine, pstat, srecv,
           lat_sem, w_sem, stat_send, stat_recv, halo_send, halo_recv):
    me = lax.axis_index("cp")
    nxt = lax.rem(me + 1, n_time)
    acts = (a0, a1, a2, a3)

    barrier = pltpu.get_barrier_semaphore()
    for d in range(1, n_time):
        pl.semaphore_signal(barrier, inc=1, device_id={"cp": lax.rem(me + d, n_time)}, device_id_type=MESH)

    def weights_copy(layer, k):
        slot = lax.rem(layer, 2)
        return pltpu.make_async_copy(w_ref.at[layer, k], wbuf.at[slot, k], w_sem.at[slot, k])

    def halo_copy(frame, par):
        return pltpu.make_async_remote_copy(
            src_ref=raw.at[frame], dst_ref=raw.at[2 + 2 * par + frame],
            send_sem=halo_send.at[frame], recv_sem=halo_recv.at[par, frame],
            device_id={"cp": nxt}, device_id_type=MESH)

    lat_copy = pltpu.make_async_copy(lat_ref, out_ref, lat_sem)
    lat_copy.start()
    weights_copy(0, 2).start()
    for n, ref in enumerate((bias_ref, gam_ref, bet_ref)):
        for layer in range(N_LAYERS):
            params[n, layer] = ref[layer:layer + 1, :]

    def cols(c):
        return slice(c * 128, (c + 1) * 128)

    def partial_sums(v):
        folded = v.reshape(v.shape[0] // 8, 8, 128)
        return jnp.sum(folded, axis=0), jnp.sum(folded * folded, axis=0)

    def latent_sums(n, carry):
        frame, row = n // ROWS, lax.rem(n, ROWS)
        new = []
        for c in range(4):
            s1, s2 = partial_sums(out_ref[frame, row, :, cols(c)].astype(F32))
            new += [carry[2 * c] + s1, carry[2 * c + 1] + s2]
        return tuple(new)

    def permute_latent(n, carry):
        frame, row = n // ROWS, lax.rem(n, ROWS)
        for c in range(4):
            perm[c] = out_ref[frame, row, :, cols(c)].astype(F32)
            for r in range(RES):
                v = perm[c, pl.ds(r, LANES, stride=RES), :].astype(BF16)
                here = (frame, row, slice(r * LANES, (r + 1) * LANES), cols(c))
                raw[here] = v
                xbuf[here] = v
        return carry

    lat_copy.wait()
    sums = lax.fori_loop(0, 2 * ROWS, latent_sums, tuple(jnp.zeros((8, 128), F32) for _ in range(8)))
    for c in range(4):
        pstat[c] = sums[2 * c]
        pstat[4 + c] = sums[2 * c + 1]

    elem_count = float(n_time * 2 * ROWS * WIDTH * (CHANS // GROUPS))
    lane = lax.broadcasted_iota(jnp.int32, (8, 128), 1)
    sub16 = lax.broadcasted_iota(jnp.int32, (LANES, 128), 0)

    def stat_copy(par, d):
        return pltpu.make_async_remote_copy(
            src_ref=srecv.at[par, me], dst_ref=srecv.at[par, me],
            send_sem=stat_send.at[d], recv_sem=stat_recv.at[par, me],
            device_id={"cp": lax.rem(me + d, n_time)}, device_id_type=MESH)

    def sums_out(par):
        for n in range(8):
            srecv[par, me, n:n + 1, :] = jnp.sum(pstat[n], axis=0, keepdims=True)
        for d in range(1, n_time):
            stat_copy(par, d).start()

    def sums_in(layer, par):

        for d in range(1, n_time):
            src = lax.rem(me + n_time - d, n_time)
            pltpu.make_async_remote_copy(
                src_ref=srecv.at[par, src], dst_ref=srecv.at[par, src],
                send_sem=stat_send.at[d], recv_sem=stat_recv.at[par, src],
                device_id={"cp": src}, device_id_type=MESH).wait_recv()

        @pl.when(layer == 0)
        def _():
            halo_copy(1, par).start()

        total = srecv[par, 0]
        for n in range(1, n_time):
            total = total + srecv[par, n]
        for s in (1, 2, 4, 8):
            total = total + jnp.where((lane & s) == 0, pltpu.roll(total, 128 - s, 1), pltpu.roll(total, s, 1))
        grp_mean = total[0:4] / elem_count
        grp_var = total[4:8] / elem_count - grp_mean * grp_mean
        inv = lax.rsqrt(grp_var + NORM_EPS)
        for c in range(4):
            scale = inv[c:c + 1] * params[1, layer, :, cols(c)]
            affine[c:c + 1, :] = scale
            affine[4 + c:5 + c, :] = params[2, layer, :, cols(c)] - grp_mean[c:c + 1] * scale
        for d in range(1, n_time):
            stat_copy(par, d).wait_send()

    pl.semaphore_wait(barrier, n_time - 1)
    sums_out(0)
    weights_copy(0, 1).start()
    weights_copy(0, 0).start()
    lax.fori_loop(0, 2 * ROWS, permute_latent, 0)

    def norm_row(slot, row, dst):
        for c in range(4):
            v = raw[slot, row, :, cols(c)].astype(F32)
            u = (v * affine[c:c + 1, :] + affine[4 + c:5 + c, :]).astype(BF16).astype(F32)
            act = u * jax.nn.sigmoid(u)
            dst[row, LANES:LANES + WIDTH, cols(c)] = act.astype(BF16)
            before = pltpu.roll(act[WIDTH - LANES:], 1, 0)
            dst[row, 0:LANES, cols(c)] = jnp.where(sub16 == 0, 0.0, before).astype(BF16)
            after = pltpu.roll(act[:LANES], LANES - 1, 0)
            dst[row, LANES + WIDTH:, cols(c)] = jnp.where(sub16 == LANES - 1, 0.0, after).astype(BF16)

    def group(acc, act, w_slot, k, first, side=None, parts=1):
        side = side or {}
        height = ROWS // parts
        steps = [(part, di) for part in range(parts) for di in (1, 0, 2)]
        for n, (part, di) in enumerate(steps):
            lo, hi = max(height * part, 1 - di), min(height * (part + 1), ROWS + 1 - di)
            lhs = jnp.concatenate(
                [act[lo + di - 1:hi + di - 1, LANES * dj:LANES * dj + WIDTH, :].reshape((hi - lo) * WIDTH, CHANS)
                 for dj in range(3)], axis=1)
            prod = jnp.dot(lhs, wbuf[w_slot, k, di].reshape(3 * CHANS, CHANS), preferred_element_type=F32)
            prod = prod.reshape(hi - lo, WIDTH, CHANS)
            if first and di == 1:
                acc[lo:hi] = prod
            else:
                acc[lo:hi] = acc[lo:hi] + prod
            for step in side.get(n, ()):
                step()

    def epilogue(frame, row, acc, layer, odd, sums):
        for q in range(2):
            for half in range(2):
                c = 2 * q + half
                h = (acc[row, :, cols(c)] + params[0, layer, :, cols(c)]).astype(BF16).astype(F32)
                x_old = xbuf[frame, row, :, cols(c)].astype(F32)
                res = (jnp.where(odd, x_old, 0.0) + h).astype(BF16)
                wide = res.astype(F32)
                raw[frame, row, :, cols(c)] = res
                xbuf[frame, row, :, cols(c)] = jnp.where(odd, wide, x_old).astype(BF16)
                s1, s2 = partial_sums(wide)
                sums[c] = s1 if sums[c] is None else sums[c] + s1
                sums[4 + c] = s2 if sums[4 + c] is None else sums[4 + c] + s2

    def layer_body(layer, carry):
        par = lax.rem(layer, 2)
        odd = par == 1
        more = layer + 1 < N_LAYERS
        later = layer > 0
        halo_0 = jnp.where(me == 0, 0, 2 + 2 * par)
        halo_1 = jnp.where(me == 0, 0, 3 + 2 * par)

        sums_in(layer, par)
        for k in (2, 1, 0):
            weights_copy(layer, k).wait()

        @pl.when(more)
        def _():
            for k in (2, 1, 0):
                weights_copy(layer + 1, k).start()

        for row in range(4):
            norm_row(1, row, a3)
        halo_copy(0, par).start()

        def normed(slot, dst, plan):
            return {n: [lambda r=r: norm_row(slot, r, dst) for r in rows] for n, rows in plan.items()}

        def finished(frame, acc, sums, plan):
            return {n: [lambda r=r: epilogue(frame, r, acc, layer, odd, sums) for r in rows] for n, rows in plan.items()}

        side = normed(0, a2, {1: (0,), 2: (1,), 3: (2,), 4: (3, 4), 5: (5,)})
        side[0] = [lambda r=r: norm_row(1, r, a3) for r in (4, 5)]
        group(acc1, a3, par, 2, True, side, 2)
        @pl.when(later)
        def _():
            halo_copy(1, par).wait_recv()

        group(acc1, a2, par, 1, False, normed(jnp.where(later, halo_1, 0), a1, {0: (0, 1), 1: (2, 3), 2: (4, 5)}))

        @pl.when(layer == 0)
        def _():
            halo_copy(1, par).wait_recv()

            def row_step(row, carry):
                norm_row(halo_1, row, a1)
                return carry

            lax.fori_loop(0, ROWS, row_step, 0)

        halo_copy(1, par).wait_send()
        sums = [None] * 8
        group(acc1, a1, par, 0, False, finished(1, acc1, sums, {3: (0,), 4: (1,), 5: (2,)}), 2)

        def finish_frame_1():
            for row in (3, 4, 5):
                epilogue(1, row, acc1, layer, odd, sums)
            for n in range(8):
                pstat[n] = sums[n]

            @pl.when(more)
            def _():
                halo_copy(1, 1 - par).start()

        group(acc0, a2, par, 2, True, {0: [finish_frame_1]})
        halo_copy(0, par).wait()
        group(acc0, a1, par, 1, False, normed(halo_0, a0, {0: (0, 1), 1: (2, 3), 2: (4, 5)}))
        sums_0 = [None] * 8
        group(acc0, a0, par, 0, False, finished(0, acc0, sums_0, {3: (0,), 4: (1,), 5: (2,)}), 2)
        for row in (3, 4, 5):
            epilogue(0, row, acc0, layer, odd, sums_0)
        for n in range(8):
            pstat[n] = pstat[n] + sums_0[n]

        @pl.when(more)
        def _():
            sums_out(1 - par)

        return carry

    lax.fori_loop(0, N_LAYERS, layer_body, 0)

    out_ref[...] = raw[0:2]


def unpermute(in_ref, out_ref, perm, rows, sems):
    def cols(c):
        return slice(c * 128, (c + 1) * 128)

    def row_copy(n):
        return pltpu.make_async_copy(rows.at[n], out_ref.at[n // ROWS, n % ROWS], sems.at[n])

    def store_row(n, carry):
        frame, row = n // ROWS, lax.rem(n, ROWS)
        for c in range(4):
            for r in range(RES):
                perm[c, pl.ds(r, LANES, stride=RES), :] = in_ref[frame, row, r * LANES:(r + 1) * LANES, cols(c)].astype(F32)
            rows[n, :, cols(c)] = perm[c].astype(BF16)
        row_copy(n).start()
        return carry

    lax.fori_loop(0, 2 * ROWS, store_row, 0)
    for n in range(2 * ROWS):
        row_copy(n).wait()


def solution(mesh):
    n_time = mesh.shape["cp"]
    frame_spec = P(("dp", "cp"))

    def local_fn(latent, conv_kernels, conv_biases, gn_gammas, gn_betas):
        act = pltpu.VMEM((ROWS, WIDTH + 2 * LANES, CHANS), BF16)
        any_spec = pl.BlockSpec(memory_space=pl.ANY)
        vmem_spec = pl.BlockSpec(memory_space=pltpu.VMEM)

        def run(*refs):
            return kernel(n_time, *refs)

        permuted = pl.pallas_call(
            run,
            out_shape=jax.ShapeDtypeStruct((2, ROWS, WIDTH, CHANS), BF16),
            in_specs=[any_spec, any_spec, vmem_spec, vmem_spec, vmem_spec],
            out_specs=vmem_spec,
            scratch_shapes=[
                pltpu.VMEM((6, ROWS, WIDTH, CHANS), BF16),
                pltpu.VMEM((2, ROWS, WIDTH, CHANS), BF16),
                pltpu.VMEM((ROWS, WIDTH, CHANS), F32),
                pltpu.VMEM((ROWS, WIDTH, CHANS), F32),
                act, act, act, act,
                pltpu.VMEM((2, 3, 3, 3, CHANS, CHANS), BF16),
                pltpu.VMEM((4, WIDTH, 128), F32),
                pltpu.VMEM((3, N_LAYERS, 1, CHANS), F32),
                pltpu.VMEM((8, 128), F32),
                pltpu.VMEM((8, 8, 128), F32),
                pltpu.VMEM((2, n_time, 8, 128), F32),
                pltpu.SemaphoreType.DMA,
                pltpu.SemaphoreType.DMA((2, 3)),
                pltpu.SemaphoreType.DMA((n_time,)),
                pltpu.SemaphoreType.DMA((2, n_time)),
                pltpu.SemaphoreType.DMA((2,)),
                pltpu.SemaphoreType.DMA((2, 2)),
            ],
            compiler_params=pltpu.CompilerParams(
                collective_id=0, has_side_effects=True, vmem_limit_bytes=60 * 1024 * 1024),
            name="resnet_blocks",
        )(latent, conv_kernels, conv_biases, gn_gammas, gn_betas)
        return pl.pallas_call(
            unpermute,
            out_shape=jax.ShapeDtypeStruct((2, ROWS, WIDTH, CHANS), BF16),
            in_specs=[vmem_spec],
            out_specs=any_spec,
            scratch_shapes=[
                pltpu.VMEM((4, WIDTH, 128), F32),
                pltpu.VMEM((2 * ROWS, WIDTH, CHANS), BF16),
                pltpu.SemaphoreType.DMA((2 * ROWS,)),
            ],
            name="unpermute",
        )(permuted)

    return jax.shard_map(local_fn, mesh=mesh, in_specs=(frame_spec, P(), P(), P(), P()), out_specs=frame_spec, check_vma=False)
```
